32 devices in a mesh: row: 4 (over y, x), col: 8 (over z, core).
Axes of the slice: x: 2, y: 2, z: 4, core: 2. Of those that a mesh axis runs over, the one named last changes fastest.
Arguments:
- out_grad: bfloat16 [4096, 512], P('col', 'row'), may hold values from -6 to 6
- node_in: bfloat16 [4096, 512], P(('row', 'col')), may hold values from -0.09375 to 0.09375
- weights: bfloat16 [3, 512, 512], replicated, may hold values from -0.25 to 0.25
- tile_vals: bfloat16 [3, 8, 4, 32, 128, 128], P(None, 'col', 'row'), may hold values from -0.15625 to 0.15625
- tile_rows: int32 [3, 8, 4, 32], P(None, 'col', 'row'), may hold values from 0 to 3
- tile_cols: int32 [3, 8, 4, 32], P(None, 'col', 'row'), may hold values from 0 to 7
- tile_count: int32 [3, 8, 4], P(None, 'col', 'row'), may hold values from 1 to 32, as said below
Outputs:
- d_nodes: bfloat16 [4096, 512], P(('row', 'col'))
- d_weights: float32 [3, 512, 512], replicated
The draws below stay inside these ranges and needn't reach their ends.
Inputs may be any that keep to these rules, and one draw needn't show every extreme that they name: Only the first tile_count slots of a block's list hold tiles; later slots are ignored. In every relation some block uses all 32 slots. `tile_rows`: coordinates may repeat within a block's list; such tiles add.
All inputs are finite; a program needn't handle non-finite values.
Results may differ from the reference program's by a relative error of at most 0.005.
Values may be sent and summed in bfloat16 or wider, within the bound.
A program may use at most 256 MiB of HBM per device.

```python
import jax
import jax.numpy as jnp
from jax import lax

D = 512
R = 3
TILE = 128
N_DEV = 128
CAP = 32
ROW_GROUPS = 4
COL_GROUPS = 8
NODES = 4096
TR = 4
TC = 8


def draw_tile_count(key, part):
    grid_shape = (R, COL_GROUPS, ROW_GROUPS)
    levels = jax.random.randint(jax.random.fold_in(key, 11), grid_shape, 1, 9)
    counts = jnp.maximum(1, CAP * levels * levels // 64)
    full_device = jax.random.randint(jax.random.fold_in(key, 12), (R,), 0, COL_GROUPS * ROW_GROUPS)
    flat_counts = counts.reshape(R, COL_GROUPS * ROW_GROUPS)
    chosen = jnp.arange(COL_GROUPS * ROW_GROUPS)[None, :] == full_device[:, None]
    flat_counts = jnp.where(chosen, CAP, flat_counts)
    return flat_counts.reshape(grid_shape).astype(jnp.int32)


def touch_ends(array, own_key, least, largest):
    extent = array.shape
    place = [jax.random.randint(jax.random.fold_in(own_key, axis), (), 0, extent[axis]) for axis in range(len(extent))]
    array = array.at[tuple(place)].set(least)
    longest = extent.index(max(extent))
    place[longest] = (place[longest] + 1) % extent[longest]
    return array.at[tuple(place)].set(largest)


def shard_levels(rng, shape, cuts, low, largest):
    def one(position, blocks):
        draws = jax.random.uniform(jax.random.fold_in(jax.random.fold_in(rng, 6), position), (blocks,), jnp.float32, low / len(cuts), largest / len(cuts))
        return jnp.repeat(jnp.exp(draws), shape[position] // blocks).reshape((-1,) + (1,) * (len(shape) - position - 1))

    loudness = one(*cuts[0])
    for cut in cuts[1:]:
        loudness = loudness * one(*cut)
    return loudness


def bell_draw(stream_key, dims, spread, most, split=(), held_as=jnp.bfloat16):
    drawn = spread * jax.random.normal(stream_key, dims, jnp.float32)
    if split:
        drawn = drawn * shard_levels(stream_key, dims, split, -0.22, 0.18)
    return jnp.clip(drawn, -most, most).astype(held_as)


def setup_inputs(seed: int = 0) -> dict:
    streams_of = jax.random.split(jax.random.key(seed), 8)
    out_grad = bell_draw(streams_of[0], (NODES, D), 1.0, 6.0, ((0, 8), (1, 4)))
    node_in = bell_draw(streams_of[1], (NODES, D), NODES ** -0.5, 0.09375, ((0, 32),))
    weights = bell_draw(streams_of[2], (R, D, D), D ** -0.5, 0.25)
    tile_vals = bell_draw(streams_of[3], (R, COL_GROUPS, ROW_GROUPS, CAP, TILE, TILE), (CAP * COL_GROUPS * 2 * TILE // (5 * TC)) ** -0.5, 0.15625, ((1, 8), (2, 4)))
    tile_rows = touch_ends(jax.random.randint(streams_of[4], (R, COL_GROUPS, ROW_GROUPS, CAP), 0, TR), jax.random.fold_in(streams_of[4], 1), 0, TR - 1).astype(jnp.int32)
    tile_cols = touch_ends(jax.random.randint(streams_of[5], (R, COL_GROUPS, ROW_GROUPS, CAP), 0, TC), jax.random.fold_in(streams_of[5], 1), 0, TC - 1).astype(jnp.int32)
    tile_count = draw_tile_count(jax.random.fold_in(streams_of[7], 71), 0)
    return {"out_grad": out_grad, "node_in": node_in, "weights": weights, "tile_vals": tile_vals, "tile_rows": tile_rows, "tile_cols": tile_cols, "tile_count": tile_count}


def block_products(operand, tile_block, row_ids, col_ids, count_now, block_index):
    group_col = block_index // ROW_GROUPS
    group_row = block_index % ROW_GROUPS
    lanes = jnp.arange(TILE, dtype=jnp.int32)
    source_ids = (group_col * (N_DEV * ROW_GROUPS) + row_ids[:, None] * TILE + lanes[None, :]).astype(jnp.int32)
    sources = jnp.take(operand, source_ids.reshape(-1), axis=0).reshape(CAP, TILE, 2 * D)
    live = (jnp.arange(CAP, dtype=jnp.int32) < count_now).astype(jnp.float32)
    products = jnp.einsum("skt,skd->std", tile_block.astype(jnp.float32), sources.astype(jnp.float32), precision=lax.Precision.HIGHEST)
    products = products * live[:, None, None]
    target_ids = (group_row * (N_DEV * COL_GROUPS) + col_ids[:, None] * TILE + lanes[None, :]).astype(jnp.int32)
    return target_ids.reshape(-1), products.reshape(CAP * TILE, 2 * D)


def reference(out_grad, node_in, weights, tile_vals, tile_rows, tile_cols, tile_count):
    blocks = COL_GROUPS * ROW_GROUPS
    block_ids = jnp.arange(blocks, dtype=jnp.int32)
    mixed_total = jnp.zeros((NODES, D), jnp.float32)
    weight_grads = []
    inputs_wide = node_in.astype(jnp.float32)
    for relation in range(R):
        premixed = jnp.dot(out_grad, weights[relation].T, preferred_element_type=jnp.float32).astype(jnp.bfloat16)
        operand = jnp.concatenate([out_grad, premixed], axis=1)

        def block_step(summed, inputs):
            target_ids, products = block_products(operand, inputs[0], inputs[1], inputs[2], inputs[3], inputs[4])
            return summed.at[target_ids].add(products), None

        scanned = (tile_vals[relation].reshape(blocks, CAP, TILE, TILE), tile_rows[relation].reshape(blocks, CAP), tile_cols[relation].reshape(blocks, CAP), tile_count[relation].reshape(blocks), block_ids)
        start_sums = jnp.zeros((NODES, 2 * D), jnp.float32)
        summed, ignored = lax.scan(block_step, start_sums, scanned)
        weight_grads.append(jnp.dot(inputs_wide.T, summed[:, :D], precision=lax.Precision.HIGHEST))
        mixed_total = mixed_total + summed[:, D:]
    return mixed_total.astype(jnp.bfloat16), jnp.stack(weight_grads)
```

```python
import functools

import jax
import jax.numpy as jnp
from jax import lax
from jax.experimental import pallas as pl
from jax.experimental.pallas import tpu as pltpu
from jax.sharding import PartitionSpec as P

MESH = pl.DeviceIdType.MESH
F32 = jnp.float32
BF16 = jnp.bfloat16


def assemble_kernel(rows_ref, cols_ref, count_ref, tiles_ref, out_ref, total):
    relation = pl.program_id(0)
    tile_rows, tile_cols, tile = total.shape[0], total.shape[1], total.shape[2]
    for i in range(tile_rows):
        for j in range(tile_cols):
            total[i, j] = jnp.zeros((tile, tile), F32)

    def add_tile(slot, carry):
        i = rows_ref[relation, slot]
        j = cols_ref[relation, slot]
        total[i, j] = total[i, j] + tiles_ref[0, slot].astype(F32)
        return carry

    lax.fori_loop(0, count_ref[relation], add_tile, 0)
    for i in range(tile_rows):
        for j in range(tile_cols):
            out_ref[i * tile : (i + 1) * tile, j * tile : (j + 1) * tile] = total[i, j].astype(BF16)


def assemble(tile_vals, tile_rows, tile_cols, tile_count, targets, sources):
    relations, cap, tile = tile_vals.shape[0], tile_vals.shape[3], tile_vals.shape[4]
    vals = tile_vals.reshape(relations, cap, tile, tile)
    return pl.pallas_call(
        assemble_kernel,
        grid_spec=pltpu.PrefetchScalarGridSpec(
            num_scalar_prefetch=3,
            grid=(relations,),
            in_specs=[pl.BlockSpec((1, cap, tile, tile), lambda r, *_: (r, 0, 0, 0))],
            out_specs=pl.BlockSpec((targets, sources), lambda r, *_: (r, 0)),
            scratch_shapes=[pltpu.VMEM((targets // tile, sources // tile, tile, tile), F32)],
        ),
        out_shape=jax.ShapeDtypeStruct((relations * targets, sources), BF16),
        compiler_params=pltpu.CompilerParams(vmem_limit_bytes=60 * 2**20),
    )(
        tile_rows.reshape(relations, cap),
        tile_cols.reshape(relations, cap),
        tile_count.reshape(relations),
        vals,
    )


def main_kernel(
    nr, nc, relations,
    grad_ref, nodes_ref, w_hbm, a_hbm,
    dn_ref, ag_ref,
    gslot, g, w, a, xall, pt, nsend, nrecv, ncomb, ndst,
    dw, dwrecv, pbuf, precv, zbuf, zrecv,
    load_sem, gs, gr, xs, xr, fs, fr, ns, nrs, nzs, nzr, ds, dr, ps, pr, zs, zr,
    azs, azr, aps, apr, acs, acr,
):
    nz = nc // 2
    tn = grad_ref.shape[0]
    width = grad_ref.shape[1]
    nd = nodes_ref.shape[0]
    f = w_hbm.shape[1]
    me_r = lax.axis_index("row")
    me_c = lax.axis_index("col")
    z = me_c // 2
    core = me_c % 2
    other = 1 - core
    sibling = {"col": z * 2 + other}

    def row_peer(d):
        return {"row": lax.rem(me_r + d, nr)}

    def z_peer(d):
        return {"col": lax.rem(z + d, nz) * 2 + core}

    def remote(src, dst, send, recv, dev):
        return pltpu.make_async_remote_copy(
            src_ref=src, dst_ref=dst, send_sem=send, recv_sem=recv, device_id=dev, device_id_type=MESH
        )

    def x_slot(k):
        return xall.at[pl.ds(pl.multiple_of(k * nd, nd), nd), :]

    load_a = pltpu.make_async_copy(a_hbm, a, load_sem.at[0])
    load_w = pltpu.make_async_copy(w_hbm, w, load_sem.at[1])
    load_w.start()
    load_a.start()

    barrier = pltpu.get_barrier_semaphore()
    for d in range(1, nr):
        pl.semaphore_signal(barrier, inc=1, device_id=row_peer(d), device_id_type=MESH)
    for d in range(1, nz):
        pl.semaphore_signal(barrier, inc=1, device_id=z_peer(d), device_id_type=MESH)
    pl.semaphore_signal(barrier, inc=1, device_id=sibling, device_id_type=MESH)
    pl.semaphore_wait(barrier, nr - 1 + nz - 1 + 1)

    g_copies = [
        remote(grad_ref, gslot.at[me_r], gs.at[d - 1], gr.at[d - 1], row_peer(d)) for d in range(1, nr)
    ]
    for c in g_copies:
        c.start()
    x_copies = [
        remote(nodes_ref, x_slot(me_c), xs.at[d - 1], xr.at[d - 1], z_peer(d)) for d in range(1, nz)
    ]
    for c in x_copies:
        c.start()
    f_copies = [remote(nodes_ref, x_slot(me_c), fs.at[0], fr.at[0], sibling)]
    f_copies[0].start()
    xall[pl.ds(pl.multiple_of(me_c * nd, nd), nd), :] = nodes_ref[...]
    gslot[me_r] = grad_ref[...]

    load_w.wait()
    for c in g_copies:
        c.wait_recv()
    for k in range(nr):
        g[:, k * width : (k + 1) * width] = gslot[k]
    for r in range(relations):
        pt[:, r * tn : (r + 1) * tn] = lax.dot_general(
            w[r], g[...], (((1,), (1,)), ((), ())), preferred_element_type=F32
        ).astype(BF16)
    load_a.wait()

    def mix(k, carry):
        for h in range(2):
            cols = pl.ds(pl.multiple_of((k * 2 + h) * nd, nd), nd)
            nsend[h, k] = jnp.dot(pt[...], a[:, cols], preferred_element_type=F32)
        return carry

    lax.fori_loop(0, nz, mix, 0)
    n_core = remote(nsend.at[other], nrecv, ns.at[0], nrs.at[0], sibling)
    n_core.start()

    for d in range(1, nz):
        x_copies[d - 1].wait_recv()
        slot = lax.rem(z + nz - d, nz) * 2 + core
        c = remote(x_slot(slot), x_slot(slot), fs.at[d], fr.at[d], sibling)
        c.start()
        f_copies.append(c)

    n_core.wait_recv()

    def combine(k, carry):
        ncomb[k] = (nsend[core, k] + nrecv[k]).astype(BF16)
        return carry

    lax.fori_loop(0, nz, combine, 0)
    n_copies = []
    for d in range(1, nz):
        c = remote(ncomb.at[lax.rem(z + d, nz)], ndst.at[d - 1], nzs.at[d - 1], nzr.at[d - 1], z_peer(d))
        c.start()
        n_copies.append(c)

    for c in f_copies:
        c.wait_recv()

    chunk = f // 2
    for j in range(2 * relations):
        r, h = j // 2, j % 2
        y = jnp.dot(
            a[r * tn : (r + 1) * tn, :],
            xall[:, h * chunk : (h + 1) * chunk],
            preferred_element_type=F32,
        )
        yt = y.astype(BF16).T
        at = (j % relations) * chunk
        dw[j // relations, at : at + chunk, :] = jnp.dot(yt, g[...], preferred_element_type=F32)

    d_core = remote(dw.at[other], dwrecv, ds.at[0], dr.at[0], sibling)
    d_core.start()
    d_core.wait_recv()
    plane_rows = pbuf.shape[1]
    for k in range(nr):
        rows = slice(k * plane_rows, (k + 1) * plane_rows)
        pbuf[k] = (dw[core, rows, :] + dwrecv[rows, :]).astype(BF16)
    p_copies = []
    for d in range(1, nr):
        c = remote(pbuf.at[lax.rem(me_r + d, nr)], precv.at[d - 1], ps.at[d - 1], pr.at[d - 1], row_peer(d))
        c.start()
        p_copies.append(c)

    for c in n_copies:
        c.wait_recv()
    own = nsend[core, z] + nrecv[z]
    for d in range(1, nz):
        own = own + ndst[d - 1].astype(F32)
    dn_ref[...] = own.T.astype(BF16)

    for c in p_copies:
        c.wait_recv()
    piece = zbuf.shape[1]
    for k in range(nz):
        rows = slice(k * piece, (k + 1) * piece)
        part = pbuf[me_r, rows, :].astype(F32)
        for d in range(1, nr):
            part = part + precv[d - 1, rows, :].astype(F32)
        zbuf[k] = part
    z_copies = []
    for d in range(1, nz):
        c = remote(zbuf.at[lax.rem(z + d, nz)], zrecv.at[d - 1], zs.at[d - 1], zr.at[d - 1], z_peer(d))
        c.start()
        z_copies.append(c)
    for c in z_copies:
        c.wait_recv()
    final = zbuf[z]
    for d in range(1, nz):
        final = final + zrecv[d - 1]
    ag_ref[core, me_r, z] = final.astype(BF16)

    tail = []
    mine = ag_ref.at[core, me_r, z]
    az = [remote(mine, mine, azs.at[d - 1], azr.at[d - 1], z_peer(d)) for d in range(1, nz)]
    for c in az:
        c.start()
    for c in az:
        c.wait_recv()
    mine = ag_ref.at[core, me_r]
    ap = [remote(mine, mine, aps.at[d - 1], apr.at[d - 1], row_peer(d)) for d in range(1, nr)]
    for c in ap:
        c.start()
    ac = [remote(mine, mine, acs.at[0], acr.at[0], sibling)]
    ac[0].start()
    for d in range(1, nr):
        ap[d - 1].wait_recv()
        slot = ag_ref.at[core, lax.rem(me_r + nr - d, nr)]
        c = remote(slot, slot, acs.at[d], acr.at[d], sibling)
        c.start()
        ac.append(c)
    for c in ac:
        c.wait_recv()
    for c in g_copies + x_copies + f_copies + [n_core] + n_copies + [d_core] + p_copies + z_copies + az + ap + ac:
        c.wait_send()


def body(nr, nc, out_grad, node_in, weights, tile_vals, tile_rows, tile_cols, tile_count):
    relations, f = weights.shape[0], weights.shape[1]
    tn, width = out_grad.shape
    nd = node_in.shape[0]
    sn = nd * nc
    nz = nc // 2
    half = relations * f // 2
    plane_rows = half // nr
    piece = plane_rows // nz
    dense = assemble(tile_vals, tile_rows, tile_cols, tile_count, tn, sn)
    dma = lambda n: pltpu.SemaphoreType.DMA((n,))
    vmem = pl.BlockSpec(memory_space=pltpu.VMEM)
    hbm = pl.BlockSpec(memory_space=pltpu.HBM)
    d_nodes, gathered = pl.pallas_call(
        functools.partial(main_kernel, nr, nc, relations),
        out_shape=(
            jax.ShapeDtypeStruct((nd, f), BF16),
            jax.ShapeDtypeStruct((2, nr, nz, piece, f), BF16),
        ),
        in_specs=[vmem, vmem, hbm, hbm],
        out_specs=(vmem, vmem),
        scratch_shapes=[
            pltpu.VMEM((nr, tn, width), BF16),
            pltpu.VMEM((tn, f), BF16),
            pltpu.VMEM(weights.shape, BF16),
            pltpu.VMEM((relations * tn, sn), BF16),
            pltpu.VMEM((sn, f), BF16),
            pltpu.VMEM((f, relations * tn), BF16),
            pltpu.VMEM((2, nz, f, nd), F32),
            pltpu.VMEM((nz, f, nd), F32),
            pltpu.VMEM((nz, f, nd), BF16),
            pltpu.VMEM((nz - 1, f, nd), BF16),
            pltpu.VMEM((2, half, f), F32),
            pltpu.VMEM((half, f), F32),
            pltpu.VMEM((nr, plane_rows, f), BF16),
            pltpu.VMEM((nr - 1, plane_rows, f), BF16),
            pltpu.VMEM((nz, piece, f), F32),
            pltpu.VMEM((nz - 1, piece, f), F32),
            dma(2),
            dma(nr - 1), dma(nr - 1),
            dma(nz - 1), dma(nz - 1),
            dma(nz), dma(nz),
            dma(1), dma(1),
            dma(nz - 1), dma(nz - 1),
            dma(1), dma(1),
            dma(nr - 1), dma(nr - 1),
            dma(nz - 1), dma(nz - 1),
            dma(nz - 1), dma(nz - 1),
            dma(nr - 1), dma(nr - 1),
            dma(nr), dma(nr),
        ],
        compiler_params=pltpu.CompilerParams(
            collective_id=0, has_side_effects=True, vmem_limit_bytes=67043328
        ),
    )(out_grad, node_in, weights, dense)
    d_weights = gathered.reshape(relations, f, f).astype(F32)
    return d_nodes, d_weights


def solution(mesh):
    return jax.shard_map(
        functools.partial(body, mesh.shape["row"], mesh.shape["col"]),
        mesh=mesh,
        in_specs=(
            P("col", "row"),
            P(("row", "col"), None),
            P(),
            P(None, "col", "row", None, None, None),
            P(None, "col", "row", None),
            P(None, "col", "row", None),
            P(None, "col", "row"),
        ),
        out_specs=(P(("row", "col"), None), P()),
        check_vma=False,
    )
```

```python
import functools

import jax
import jax.numpy as jnp
from jax import lax
from jax.experimental import pallas as pl
from jax.experimental.pallas import tpu as pltpu
from jax.sharding import PartitionSpec as P

MESH = pl.DeviceIdType.MESH
F32 = jnp.float32
BF16 = jnp.bfloat16


def assemble_kernel(rows_ref, cols_ref, count_ref, tiles_ref, out_ref, total):
    relation = pl.program_id(0)
    tile_rows, tile_cols, tile = total.shape[0], total.shape[1], total.shape[2]
    for i in range(tile_rows):
        for j in range(tile_cols):
            total[i, j] = jnp.zeros((tile, tile), F32)

    def add_tile(slot, carry):
        i = rows_ref[relation, slot]
        j = cols_ref[relation, slot]
        total[i, j] = total[i, j] + tiles_ref[0, slot].astype(F32)
        return carry

    lax.fori_loop(0, count_ref[relation], add_tile, 0)
    for i in range(tile_rows):
        for j in range(tile_cols):
            out_ref[i * tile : (i + 1) * tile, j * tile : (j + 1) * tile] = total[i, j].astype(BF16)


def assemble(tile_vals, tile_rows, tile_cols, tile_count, targets, sources):
    relations, cap, tile = tile_vals.shape[0], tile_vals.shape[3], tile_vals.shape[4]
    vals = tile_vals.reshape(relations, cap, tile, tile)
    return pl.pallas_call(
        assemble_kernel,
        grid_spec=pltpu.PrefetchScalarGridSpec(
            num_scalar_prefetch=3,
            grid=(relations,),
            in_specs=[pl.BlockSpec((1, cap, tile, tile), lambda r, *_: (r, 0, 0, 0))],
            out_specs=pl.BlockSpec((targets, sources), lambda r, *_: (r, 0)),
            scratch_shapes=[pltpu.VMEM((targets // tile, sources // tile, tile, tile), F32)],
        ),
        out_shape=jax.ShapeDtypeStruct((relations * targets, sources), BF16),
        compiler_params=pltpu.CompilerParams(vmem_limit_bytes=60 * 2**20),
    )(
        tile_rows.reshape(relations, cap),
        tile_cols.reshape(relations, cap),
        tile_count.reshape(relations),
        vals,
    )


def main_kernel(
    nr, nc, relations,
    grad_ref, nodes_ref, w_hbm, a_hbm,
    dn_ref, ag_ref,
    gslot, g, w, a, xall, pt, nsend, nrecv, ncomb, ndst,
    dw, dwrecv, pbuf, precv, zbuf, zrecv,
    load_sem, gs, gr, xs, xr, fs, fr, ns, nrs, nzs, nzr, ds, dr, ps, pr, zs, zr,
    azs, azr, aps, apr, acs, acr,
):
    nz = nc // 2
    tn = grad_ref.shape[0]
    width = grad_ref.shape[1]
    nd = nodes_ref.shape[0]
    f = w_hbm.shape[1]
    me_r = lax.axis_index("row")
    me_c = lax.axis_index("col")
    z = me_c // 2
    core = me_c % 2
    other = 1 - core
    sibling = {"col": z * 2 + other}

    def row_peer(d):
        return {"row": lax.rem(me_r + d, nr)}

    def z_peer(d):
        return {"col": lax.rem(z + d, nz) * 2 + core}

    def remote(src, dst, send, recv, dev):
        return pltpu.make_async_remote_copy(
            src_ref=src, dst_ref=dst, send_sem=send, recv_sem=recv, device_id=dev, device_id_type=MESH
        )

    def x_slot(k):
        return xall.at[pl.ds(pl.multiple_of(k * nd, nd), nd), :]

    load_a = pltpu.make_async_copy(a_hbm, a, load_sem.at[0])
    load_w = pltpu.make_async_copy(w_hbm, w, load_sem.at[1])
    load_w.start()
    load_a.start()

    barrier = pltpu.get_barrier_semaphore()
    for d in range(1, nr):
        pl.semaphore_signal(barrier, inc=1, device_id=row_peer(d), device_id_type=MESH)
    for d in range(1, nz):
        pl.semaphore_signal(barrier, inc=1, device_id=z_peer(d), device_id_type=MESH)
    pl.semaphore_signal(barrier, inc=1, device_id=sibling, device_id_type=MESH)
    pl.semaphore_wait(barrier, nr - 1 + nz - 1 + 1)

    g_copies = [
        remote(grad_ref, gslot.at[me_r], gs.at[d - 1], gr.at[d - 1], row_peer(d)) for d in range(1, nr)
    ]
    for c in g_copies:
        c.start()
    x_copies = [
        remote(nodes_ref, x_slot(me_c), xs.at[d - 1], xr.at[d - 1], z_peer(d)) for d in range(1, nz)
    ]
    for c in x_copies:
        c.start()
    f_copies = [remote(nodes_ref, x_slot(me_c), fs.at[0], fr.at[0], sibling)]
    f_copies[0].start()
    xall[pl.ds(pl.multiple_of(me_c * nd, nd), nd), :] = nodes_ref[...]
    gslot[me_r] = grad_ref[...]

    load_w.wait()
    for c in g_copies:
        c.wait_recv()
    for k in range(nr):
        g[:, k * width : (k + 1) * width] = gslot[k]
    for r in range(relations):
        pt[:, r * tn : (r + 1) * tn] = lax.dot_general(
            w[r], g[...], (((1,), (1,)), ((), ())), preferred_element_type=F32
        ).astype(BF16)
    load_a.wait()

    def mix(k, carry):
        for h in range(2):
            cols = pl.ds(pl.multiple_of((k * 2 + h) * nd, nd), nd)
            nsend[h, k] = jnp.dot(pt[...], a[:, cols], preferred_element_type=F32)
        return carry

    lax.fori_loop(0, nz, mix, 0)
    n_core = remote(nsend.at[other], nrecv, ns.at[0], nrs.at[0], sibling)
    n_core.start()

    for d in range(1, nz):
        x_copies[d - 1].wait_recv()
        slot = lax.rem(z + nz - d, nz) * 2 + core
        c = remote(x_slot(slot), x_slot(slot), fs.at[d], fr.at[d], sibling)
        c.start()
        f_copies.append(c)

    n_core.wait_recv()

    def combine(k, carry):
        ncomb[k] = (nsend[core, k] + nrecv[k]).astype(BF16)
        return carry

    lax.fori_loop(0, nz, combine, 0)
    n_copies = [
        remote(ncomb.at[lax.rem(z + d, nz)], ndst.at[d - 1], nzs.at[d - 1], nzr.at[d - 1], z_peer(d))
        for d in range(1, nz)
    ]
    for c in n_copies[:-1]:
        c.start()

    for c in f_copies:
        c.wait_recv()

    chunk = f // 2
    plane_rows = pbuf.shape[2]
    piece = zbuf.shape[2]
    sent = [[] for _ in range(relations)]
    batches = [[None] * relations for _ in range(5)]

    def launch(stage, r, copies):
        for c in copies:
            c.start()
        batches[stage][r] = copies
        sent[r].extend(copies)

    def arrived(stage, r):
        for c in batches[stage][r]:
            c.wait_recv()

    def terms(r):
        for h in range(2):
            y = jnp.dot(
                a[r * tn : (r + 1) * tn, :],
                xall[:, h * chunk : (h + 1) * chunk],
                preferred_element_type=F32,
            )
            dw[r, h] = jnp.dot(y.astype(BF16).T, g[...], preferred_element_type=F32)
        launch(0, r, [remote(dw.at[r, other], dwrecv.at[r], ds.at[r, 0], dr.at[r, 0], sibling)])

    def plane_scatter(r):
        arrived(0, r)
        for k in range(nr):
            rows = slice(k * plane_rows, (k + 1) * plane_rows)
            pbuf[r, k] = (dw[r, core, rows, :] + dwrecv[r, rows, :]).astype(BF16)
        launch(1, r, [
            remote(
                pbuf.at[r, lax.rem(me_r + d, nr)], precv.at[r, d - 1],
                ps.at[r, d - 1], pr.at[r, d - 1], row_peer(d),
            )
            for d in range(1, nr)
        ])

    def z_scatter(r):
        arrived(1, r)
        for k in range(nz):
            rows = slice(k * piece, (k + 1) * piece)
            part = pbuf[r, me_r, rows, :].astype(F32)
            for d in range(1, nr):
                part = part + precv[r, d - 1, rows, :].astype(F32)
            zbuf[r, k] = part.astype(BF16)
        launch(2, r, [
            remote(
                zbuf.at[r, lax.rem(z + d, nz)], zrecv.at[r, d - 1],
                zs.at[r, d - 1], zr.at[r, d - 1], z_peer(d),
            )
            for d in range(1, nz)
        ])

    def z_gather(r):
        arrived(2, r)
        final = zbuf[r, z].astype(F32)
        for d in range(1, nz):
            final = final + zrecv[r, d - 1].astype(F32)
        ag_ref[r, core, me_r, z] = final.astype(BF16)
        mine = ag_ref.at[r, core, me_r, z]
        launch(3, r, [remote(mine, mine, azs.at[r, d - 1], azr.at[r, d - 1], z_peer(d)) for d in range(1, nz)])

    last = [[] for _ in range(relations)]

    def plane_gather(r):
        arrived(3, r)
        mine = ag_ref.at[r, core, me_r]
        launch(4, r, [remote(mine, mine, aps.at[r, d - 1], apr.at[r, d - 1], row_peer(d)) for d in range(1, nr)])
        c = remote(mine, mine, acs.at[r, 0], acr.at[r, 0], sibling)
        c.start()
        last[r].append(c)

    def core_gather(r):
        for d in range(1, nr):
            batches[4][r][d - 1].wait_recv()
            slot = ag_ref.at[r, core, lax.rem(me_r + nr - d, nr)]
            c = remote(slot, slot, acs.at[r, d], acr.at[r, d], sibling)
            c.start()
            last[r].append(c)

    terms(0)
    for r in range(1, relations):
        terms(r)
        plane_scatter(r - 1)
    plane_scatter(relations - 1)
    stages = (z_scatter, z_gather, plane_gather, core_gather)
    for t in range(relations + len(stages) - 1):
        for stage in reversed(range(len(stages))):
            if 0 <= t - stage < relations:
                stages[stage](t - stage)
        if t == relations:
            n_copies[-1].start()

    for c in n_copies:
        c.wait_recv()
    own = nsend[core, z] + nrecv[z]
    for d in range(1, nz):
        own = own + ndst[d - 1].astype(F32)
    dn_ref[...] = own.T.astype(BF16)

    for r in range(relations):
        for c in last[r]:
            c.wait_recv()
        for c in sent[r] + last[r]:
            c.wait_send()
    for c in g_copies + x_copies + f_copies + [n_core] + n_copies:
        c.wait_send()


def body(nr, nc, out_grad, node_in, weights, tile_vals, tile_rows, tile_cols, tile_count):
    relations, f = weights.shape[0], weights.shape[1]
    tn, width = out_grad.shape
    nd = node_in.shape[0]
    sn = nd * nc
    nz = nc // 2
    half = f // 2
    plane_rows = half // nr
    piece = plane_rows // nz
    dense = assemble(tile_vals, tile_rows, tile_cols, tile_count, tn, sn)
    dma = lambda *n: pltpu.SemaphoreType.DMA(n)
    vmem = pl.BlockSpec(memory_space=pltpu.VMEM)
    hbm = pl.BlockSpec(memory_space=pltpu.HBM)
    d_nodes, gathered = pl.pallas_call(
        functools.partial(main_kernel, nr, nc, relations),
        out_shape=(
            jax.ShapeDtypeStruct((nd, f), BF16),
            jax.ShapeDtypeStruct((relations, 2, nr, nz, piece, f), BF16),
        ),
        in_specs=[vmem, vmem, hbm, hbm],
        out_specs=(vmem, vmem),
        scratch_shapes=[
            pltpu.VMEM((nr, tn, width), BF16),
            pltpu.VMEM((tn, f), BF16),
            pltpu.VMEM(weights.shape, BF16),
            pltpu.VMEM((relations * tn, sn), BF16),
            pltpu.VMEM((sn, f), BF16),
            pltpu.VMEM((f, relations * tn), BF16),
            pltpu.VMEM((2, nz, f, nd), F32),
            pltpu.VMEM((nz, f, nd), F32),
            pltpu.VMEM((nz, f, nd), BF16),
            pltpu.VMEM((nz - 1, f, nd), BF16),
            pltpu.VMEM((relations, 2, half, f), F32),
            pltpu.VMEM((relations, half, f), F32),
            pltpu.VMEM((relations, nr, plane_rows, f), BF16),
            pltpu.VMEM((relations, nr - 1, plane_rows, f), BF16),
            pltpu.VMEM((relations, nz, piece, f), BF16),
            pltpu.VMEM((relations, nz - 1, piece, f), BF16),
            dma(2),
            dma(nr - 1), dma(nr - 1),
            dma(nz - 1), dma(nz - 1),
            dma(nz), dma(nz),
            dma(1), dma(1),
            dma(nz - 1), dma(nz - 1),
            dma(relations, 1), dma(relations, 1),
            dma(relations, nr - 1), dma(relations, nr - 1),
            dma(relations, nz - 1), dma(relations, nz - 1),
            dma(relations, nz - 1), dma(relations, nz - 1),
            dma(relations, nr - 1), dma(relations, nr - 1),
            dma(relations, nr), dma(relations, nr),
        ],
        compiler_params=pltpu.CompilerParams(
            collective_id=0, has_side_effects=True, vmem_limit_bytes=67043328
        ),
    )(out_grad, node_in, weights, dense)
    d_weights = gathered.reshape(relations, f, f).astype(F32)
    return d_nodes, d_weights


def solution(mesh):
    return jax.shard_map(
        functools.partial(body, mesh.shape["row"], mesh.shape["col"]),
        mesh=mesh,
        in_specs=(
            P("col", "row"),
            P(("row", "col"), None),
            P(),
            P(None, "col", "row", None, None, None),
            P(None, "col", "row", None),
            P(None, "col", "row", None),
            P(None, "col", "row"),
        ),
        out_specs=(P(("row", "col"), None), P()),
        check_vma=False,
    )
```

```python
import functools

import jax
import jax.numpy as jnp
from jax import lax
from jax.experimental import pallas as pl
from jax.experimental.pallas import tpu as pltpu
from jax.sharding import PartitionSpec as P

MESH = pl.DeviceIdType.MESH
F32 = jnp.float32
BF16 = jnp.bfloat16


def assemble_kernel(rows_ref, cols_ref, count_ref, tiles_ref, out_ref, total):
    relation = pl.program_id(0)
    tile_rows, tile_cols, tile = total.shape[0], total.shape[1], total.shape[2]
    for i in range(tile_rows):
        for j in range(tile_cols):
            total[i, j] = jnp.zeros((tile, tile), F32)

    def add_tile(slot, carry):
        i = rows_ref[relation, 0, 0, slot]
        j = cols_ref[relation, 0, 0, slot]
        total[i, j] = total[i, j] + tiles_ref[0, slot].astype(F32)
        return carry

    lax.fori_loop(0, count_ref[relation], add_tile, 0)
    for i in range(tile_rows):
        for j in range(tile_cols):
            out_ref[i * tile : (i + 1) * tile, j * tile : (j + 1) * tile] = total[i, j].astype(BF16)


def assemble(tile_vals, tile_rows, tile_cols, tile_count, targets, sources):
    relations, cap, tile = tile_vals.shape[0], tile_vals.shape[3], tile_vals.shape[4]
    vals = tile_vals.reshape(relations, cap, tile, tile)
    return pl.pallas_call(
        assemble_kernel,
        grid_spec=pltpu.PrefetchScalarGridSpec(
            num_scalar_prefetch=3,
            grid=(relations,),
            in_specs=[pl.BlockSpec((1, cap, tile, tile), lambda r, *_: (r, 0, 0, 0))],
            out_specs=pl.BlockSpec((targets, sources), lambda r, *_: (r, 0)),
            scratch_shapes=[pltpu.VMEM((targets // tile, sources // tile, tile, tile), F32)],
        ),
        out_shape=jax.ShapeDtypeStruct((relations * targets, sources), BF16),
        compiler_params=pltpu.CompilerParams(vmem_limit_bytes=60 * 2**20),
    )(
        tile_rows,
        tile_cols,
        tile_count.reshape(relations),
        vals,
    )


def main_kernel(
    nr, nc, relations,
    grad_ref, nodes_ref, w_hbm, a_hbm,
    dn_ref, ag_ref,
    gslot, g, w, a, xall, pt, nsend, nrecv, ncomb, ndst,
    dw, dwrecv, pbuf, precv, zbuf, zrecv,
    load_sem, gs, gr, xs, xr, fs, fr, ns, nrs, nzs, nzr, ds, dr, ps, pr, zs, zr,
    azs, azr, aps, apr, acs, acr,
):
    nz = nc // 2
    tn = grad_ref.shape[0]
    width = grad_ref.shape[1]
    nd = nodes_ref.shape[0]
    f = w_hbm.shape[1]
    me_r = lax.axis_index("row")
    me_c = lax.axis_index("col")
    z = me_c // 2
    core = me_c % 2
    other = 1 - core
    sibling = {"col": z * 2 + other}

    def row_peer(d):
        return {"row": lax.rem(me_r + d, nr)}

    def z_peer(d):
        return {"col": lax.rem(z + d, nz) * 2 + core}

    def remote(src, dst, send, recv, dev):
        return pltpu.make_async_remote_copy(
            src_ref=src, dst_ref=dst, send_sem=send, recv_sem=recv, device_id=dev, device_id_type=MESH
        )

    def x_slot(k):
        return xall.at[pl.ds(pl.multiple_of(k * nd, nd), nd), :]

    load_a = pltpu.make_async_copy(a_hbm, a, load_sem.at[0])
    load_w = pltpu.make_async_copy(w_hbm, w, load_sem.at[1])
    load_w.start()
    load_a.start()

    barrier = pltpu.get_barrier_semaphore()
    for d in range(1, nr):
        pl.semaphore_signal(barrier, inc=1, device_id=row_peer(d), device_id_type=MESH)
    for d in range(1, nz):
        pl.semaphore_signal(barrier, inc=1, device_id=z_peer(d), device_id_type=MESH)
    pl.semaphore_signal(barrier, inc=1, device_id=sibling, device_id_type=MESH)
    pl.semaphore_wait(barrier, nr - 1 + nz - 1 + 1)

    g_copies = [
        remote(grad_ref, gslot.at[me_r], gs.at[d - 1], gr.at[d - 1], row_peer(d)) for d in range(1, nr)
    ]
    for c in g_copies:
        c.start()
    x_copies = [
        remote(nodes_ref, x_slot(me_c), xs.at[d - 1], xr.at[d - 1], z_peer(d)) for d in range(1, nz)
    ]
    for c in x_copies:
        c.start()
    f_copies = [remote(nodes_ref, x_slot(me_c), fs.at[0], fr.at[0], sibling)]
    f_copies[0].start()
    xall[pl.ds(pl.multiple_of(me_c * nd, nd), nd), :] = nodes_ref[...]
    gslot[me_r] = grad_ref[...]

    load_w.wait()
    for c in g_copies:
        c.wait_recv()
    for k in range(nr):
        g[:, k * width : (k + 1) * width] = gslot[k]
    for r in range(relations):
        pt[:, r * tn : (r + 1) * tn] = lax.dot_general(
            w[r], g[...], (((1,), (1,)), ((), ())), preferred_element_type=F32
        ).astype(BF16)
    load_a.wait()

    def mix(k, carry):
        cols = pl.ds(pl.multiple_of(k * 2 * nd, 2 * nd), 2 * nd)
        both = jnp.dot(pt[...], a[:, cols], preferred_element_type=F32)
        nsend[0, k] = both[:, :nd]
        nsend[1, k] = both[:, nd:]
        return carry

    lax.fori_loop(0, nz, mix, 0)
    n_core = remote(nsend.at[other], nrecv, ns.at[0], nrs.at[0], sibling)
    n_core.start()

    for d in range(1, nz):
        x_copies[d - 1].wait_recv()
        slot = lax.rem(z + nz - d, nz) * 2 + core
        c = remote(x_slot(slot), x_slot(slot), fs.at[d], fr.at[d], sibling)
        c.start()
        f_copies.append(c)

    n_core.wait_recv()

    def combine(k, carry):
        ncomb[k] = (nsend[core, k] + nrecv[k]).astype(BF16)
        return carry

    lax.fori_loop(0, nz, combine, 0)
    n_copies = [
        remote(ncomb.at[lax.rem(z + d, nz)], ndst.at[d - 1], nzs.at[d - 1], nzr.at[d - 1], z_peer(d))
        for d in range(1, nz)
    ]
    for c in n_copies[:-1]:
        c.start()

    for c in f_copies:
        c.wait_recv()

    chunk = f // 2
    plane_rows = pbuf.shape[2]
    piece = zbuf.shape[2]
    sent = [[] for _ in range(relations)]
    batches = [[None] * relations for _ in range(5)]

    def launch(stage, r, copies):
        for c in copies:
            c.start()
        batches[stage][r] = copies
        sent[r].extend(copies)

    def arrived(stage, r):
        for c in batches[stage][r]:
            c.wait_recv()

    def terms(r):
        for h in range(2):
            y = jnp.dot(
                a[r * tn : (r + 1) * tn, :],
                xall[:, h * chunk : (h + 1) * chunk],
                preferred_element_type=F32,
            )
            dw[r, h] = jnp.dot(y.astype(BF16).T, g[...], preferred_element_type=F32)
        launch(0, r, [remote(dw.at[r, other], dwrecv.at[r], ds.at[r, 0], dr.at[r, 0], sibling)])

    def plane_scatter(r):
        arrived(0, r)
        for k in range(nr):
            rows = slice(k * plane_rows, (k + 1) * plane_rows)
            pbuf[r, k] = (dw[r, core, rows, :] + dwrecv[r, rows, :]).astype(BF16)
        launch(1, r, [
            remote(
                pbuf.at[r, lax.rem(me_r + d, nr)], precv.at[r, d - 1],
                ps.at[r, d - 1], pr.at[r, d - 1], row_peer(d),
            )
            for d in range(1, nr)
        ])

    def z_scatter(r):
        arrived(1, r)
        for k in range(nz):
            rows = slice(k * piece, (k + 1) * piece)
            part = pbuf[r, me_r, rows, :].astype(F32)
            for d in range(1, nr):
                part = part + precv[r, d - 1, rows, :].astype(F32)
            zbuf[r, k] = part.astype(BF16)
        launch(2, r, [
            remote(
                zbuf.at[r, lax.rem(z + d, nz)], zrecv.at[r, d - 1],
                zs.at[r, d - 1], zr.at[r, d - 1], z_peer(d),
            )
            for d in range(1, nz)
        ])

    def z_gather(r):
        arrived(2, r)
        final = zbuf[r, z].astype(F32)
        for d in range(1, nz):
            final = final + zrecv[r, d - 1].astype(F32)
        ag_ref[r, core, me_r, z] = final.astype(BF16)
        mine = ag_ref.at[r, core, me_r, z]
        launch(3, r, [remote(mine, mine, azs.at[r, d - 1], azr.at[r, d - 1], z_peer(d)) for d in range(1, nz)])

    last = [[] for _ in range(relations)]

    def plane_gather(r):
        arrived(3, r)
        mine = ag_ref.at[r, core, me_r]
        launch(4, r, [remote(mine, mine, aps.at[r, d - 1], apr.at[r, d - 1], row_peer(d)) for d in range(1, nr)])
        c = remote(mine, mine, acs.at[r, 0], acr.at[r, 0], sibling)
        c.start()
        last[r].append(c)

    def core_gather(r):
        for d in range(1, nr):
            batches[4][r][d - 1].wait_recv()
            slot = ag_ref.at[r, core, lax.rem(me_r + nr - d, nr)]
            c = remote(slot, slot, acs.at[r, d], acr.at[r, d], sibling)
            c.start()
            last[r].append(c)

    terms(0)
    for r in range(1, relations):
        terms(r)
        plane_scatter(r - 1)
    plane_scatter(relations - 1)
    stages = (z_scatter, z_gather, plane_gather, core_gather)
    for t in range(relations + len(stages) - 1):
        for stage in reversed(range(len(stages))):
            if 0 <= t - stage < relations:
                stages[stage](t - stage)
        if t == relations:
            n_copies[-1].start()

    for c in n_copies:
        c.wait_recv()
    own = nsend[core, z] + nrecv[z]
    for d in range(1, nz):
        own = own + ndst[d - 1].astype(F32)
    dn_ref[...] = own.T.astype(BF16)

    for r in range(relations):
        for c in last[r]:
            c.wait_recv()
        for c in sent[r] + last[r]:
            c.wait_send()
    for c in g_copies + x_copies + f_copies + [n_core] + n_copies:
        c.wait_send()


def widen_kernel(dn_ref, dw_ref, dn_out, dw_out):
    dn_out[...] = dn_ref[...]
    dw_out[...] = dw_ref[...].astype(F32)


def widen(d_nodes, gathered):
    relations, f = gathered.shape[0], gathered.shape[1]
    parts = 2
    weight = pl.BlockSpec((1, f // parts, f), lambda r, h: (r, h, 0))
    nodes = pl.BlockSpec(d_nodes.shape, lambda r, h: (0, 0))
    return pl.pallas_call(
        widen_kernel,
        grid=(relations, parts),
        in_specs=[nodes, weight],
        out_specs=(nodes, weight),
        out_shape=(
            jax.ShapeDtypeStruct(d_nodes.shape, BF16),
            jax.ShapeDtypeStruct(gathered.shape, F32),
        ),
    )(d_nodes, gathered)


def body(nr, nc, out_grad, node_in, weights, tile_vals, tile_rows, tile_cols, tile_count):
    relations, f = weights.shape[0], weights.shape[1]
    tn, width = out_grad.shape
    nd = node_in.shape[0]
    sn = nd * nc
    nz = nc // 2
    half = f // 2
    plane_rows = half // nr
    piece = plane_rows // nz
    dense = assemble(tile_vals, tile_rows, tile_cols, tile_count, tn, sn)
    dma = lambda *n: pltpu.SemaphoreType.DMA(n)
    vmem = pl.BlockSpec(memory_space=pltpu.VMEM)
    hbm = pl.BlockSpec(memory_space=pltpu.HBM)
    d_nodes, gathered = pl.pallas_call(
        functools.partial(main_kernel, nr, nc, relations),
        out_shape=(
            jax.ShapeDtypeStruct((nd, f), BF16),
            jax.ShapeDtypeStruct((relations, 2, nr, nz, piece, f), BF16),
        ),
        in_specs=[vmem, vmem, hbm, hbm],
        out_specs=(vmem, vmem),
        scratch_shapes=[
            pltpu.VMEM((nr, tn, width), BF16),
            pltpu.VMEM((tn, f), BF16),
            pltpu.VMEM(weights.shape, BF16),
            pltpu.VMEM((relations * tn, sn), BF16),
            pltpu.VMEM((sn, f), BF16),
            pltpu.VMEM((f, relations * tn), BF16),
            pltpu.VMEM((2, nz, f, nd), F32),
            pltpu.VMEM((nz, f, nd), F32),
            pltpu.VMEM((nz, f, nd), BF16),
            pltpu.VMEM((nz - 1, f, nd), BF16),
            pltpu.VMEM((relations, 2, half, f), F32),
            pltpu.VMEM((relations, half, f), F32),
            pltpu.VMEM((relations, nr, plane_rows, f), BF16),
            pltpu.VMEM((relations, nr - 1, plane_rows, f), BF16),
            pltpu.VMEM((relations, nz, piece, f), BF16),
            pltpu.VMEM((relations, nz - 1, piece, f), BF16),
            dma(2),
            dma(nr - 1), dma(nr - 1),
            dma(nz - 1), dma(nz - 1),
            dma(nz), dma(nz),
            dma(1), dma(1),
            dma(nz - 1), dma(nz - 1),
            dma(relations, 1), dma(relations, 1),
            dma(relations, nr - 1), dma(relations, nr - 1),
            dma(relations, nz - 1), dma(relations, nz - 1),
            dma(relations, nz - 1), dma(relations, nz - 1),
            dma(relations, nr - 1), dma(relations, nr - 1),
            dma(relations, nr), dma(relations, nr),
        ],
        compiler_params=pltpu.CompilerParams(
            collective_id=0, has_side_effects=True, vmem_limit_bytes=67043328
        ),
    )(out_grad, node_in, weights, dense)
    return widen(d_nodes, gathered.reshape(relations, f, f))


def solution(mesh):
    return jax.shard_map(
        functools.partial(body, mesh.shape["row"], mesh.shape["col"]),
        mesh=mesh,
        in_specs=(
            P("col", "row"),
            P(("row", "col"), None),
            P(),
            P(None, "col", "row", None, None, None),
            P(None, "col", "row", None),
            P(None, "col", "row", None),
            P(None, "col", "row"),
        ),
        out_specs=(P(("row", "col"), None), P()),
        check_vma=False,
    )
```

```python
import functools

import jax
import jax.numpy as jnp
from jax import lax
from jax.experimental import pallas as pl
from jax.experimental.pallas import tpu as pltpu
from jax.sharding import PartitionSpec as P

MESH = pl.DeviceIdType.MESH
F32 = jnp.float32
BF16 = jnp.bfloat16


def assemble_kernel(rows_ref, cols_ref, count_ref, tiles_ref, out_ref, total):
    relation = pl.program_id(0)
    tile_rows, tile_cols, tile = total.shape[0], total.shape[1], total.shape[2]
    for i in range(tile_rows):
        for j in range(tile_cols):
            total[i, j] = jnp.zeros((tile, tile), F32)

    def add_tile(slot, carry):
        i = rows_ref[relation, 0, 0, slot]
        j = cols_ref[relation, 0, 0, slot]
        total[i, j] = total[i, j] + tiles_ref[0, slot].astype(F32)
        return carry

    lax.fori_loop(0, count_ref[relation], add_tile, 0)
    for i in range(tile_rows):
        for j in range(tile_cols):
            out_ref[i * tile : (i + 1) * tile, j * tile : (j + 1) * tile] = total[i, j].astype(BF16)


def assemble(tile_vals, tile_rows, tile_cols, tile_count, targets, sources):
    relations, cap, tile = tile_vals.shape[0], tile_vals.shape[3], tile_vals.shape[4]
    vals = tile_vals.reshape(relations, cap, tile, tile)
    return pl.pallas_call(
        assemble_kernel,
        grid_spec=pltpu.PrefetchScalarGridSpec(
            num_scalar_prefetch=3,
            grid=(relations,),
            in_specs=[pl.BlockSpec((1, cap, tile, tile), lambda r, *_: (r, 0, 0, 0))],
            out_specs=pl.BlockSpec((targets, sources), lambda r, *_: (r, 0)),
            scratch_shapes=[pltpu.VMEM((targets // tile, sources // tile, tile, tile), F32)],
        ),
        out_shape=jax.ShapeDtypeStruct((relations * targets, sources), BF16),
        compiler_params=pltpu.CompilerParams(vmem_limit_bytes=60 * 2**20),
    )(
        tile_rows,
        tile_cols,
        tile_count.reshape(relations),
        vals,
    )


def main_kernel(
    nr, nc, relations,
    grad_ref, nodes_ref, w_hbm, a_hbm,
    dn_ref, ag_ref,
    gslot, g, w, a, xall, pt, nsend, nrecv, ncomb, ndst,
    dw, dwrecv, pbuf, precv, zbuf, zrecv,
    load_sem, gs, gr, xs, xr, fs, fr, ns, nrs, nzs, nzr, ds, dr, ps, pr, zs, zr,
    azs, azr, aps, apr, acs, acr,
):
    nz = nc // 2
    tn = grad_ref.shape[0]
    width = grad_ref.shape[1]
    nd = nodes_ref.shape[0]
    f = w_hbm.shape[1]
    me_r = lax.axis_index("row")
    me_c = lax.axis_index("col")
    z = me_c // 2
    core = me_c % 2
    other = 1 - core
    sibling = {"col": z * 2 + other}

    def row_peer(d):
        return {"row": lax.rem(me_r + d, nr)}

    def z_peer(d):
        return {"col": lax.rem(z + d, nz) * 2 + core}

    def remote(src, dst, send, recv, dev):
        return pltpu.make_async_remote_copy(
            src_ref=src, dst_ref=dst, send_sem=send, recv_sem=recv, device_id=dev, device_id_type=MESH
        )

    def x_slot(k):
        return xall.at[pl.ds(pl.multiple_of(k * nd, nd), nd), :]

    load_a = pltpu.make_async_copy(a_hbm, a, load_sem.at[0])
    load_w = pltpu.make_async_copy(w_hbm, w, load_sem.at[1])
    load_w.start()
    load_a.start()

    barrier = pltpu.get_barrier_semaphore()
    for d in range(1, nr):
        pl.semaphore_signal(barrier, inc=1, device_id=row_peer(d), device_id_type=MESH)
    for d in range(1, nz):
        pl.semaphore_signal(barrier, inc=1, device_id=z_peer(d), device_id_type=MESH)
    pl.semaphore_signal(barrier, inc=1, device_id=sibling, device_id_type=MESH)
    pl.semaphore_wait(barrier, nr - 1 + nz - 1 + 1)

    g_copies = [
        remote(grad_ref, gslot.at[me_r], gs.at[d - 1], gr.at[d - 1], row_peer(d)) for d in range(1, nr)
    ]
    for c in g_copies:
        c.start()
    x_copies = [
        remote(nodes_ref, x_slot(me_c), xs.at[d - 1], xr.at[d - 1], z_peer(d)) for d in range(1, nz)
    ]
    for c in x_copies:
        c.start()
    f_copies = [remote(nodes_ref, x_slot(me_c), fs.at[0], fr.at[0], sibling)]
    f_copies[0].start()
    xall[pl.ds(pl.multiple_of(me_c * nd, nd), nd), :] = nodes_ref[...]
    gslot[me_r] = grad_ref[...]

    load_w.wait()
    for c in g_copies:
        c.wait_recv()
    for k in range(nr):
        g[:, k * width : (k + 1) * width] = gslot[k]
    for r in range(relations):
        pt[:, r * tn : (r + 1) * tn] = lax.dot_general(
            w[r], g[...], (((1,), (1,)), ((), ())), preferred_element_type=F32
        ).astype(BF16)
    load_a.wait()

    def mix(k, carry):
        cols = pl.ds(pl.multiple_of(k * 2 * nd, 2 * nd), 2 * nd)
        both = jnp.dot(pt[...], a[:, cols], preferred_element_type=F32)
        nsend[0, k] = both[:, :nd]
        nsend[1, k] = both[:, nd:]
        return carry

    lax.fori_loop(0, nz, mix, 0)
    n_core = remote(nsend.at[other], nrecv, ns.at[0], nrs.at[0], sibling)
    n_core.start()

    for d in range(1, nz):
        x_copies[d - 1].wait_recv()
        slot = lax.rem(z + nz - d, nz) * 2 + core
        c = remote(x_slot(slot), x_slot(slot), fs.at[d], fr.at[d], sibling)
        c.start()
        f_copies.append(c)

    n_core.wait_recv()

    def combine(k, carry):
        ncomb[k] = (nsend[core, k] + nrecv[k]).astype(BF16)
        return carry

    lax.fori_loop(0, nz, combine, 0)
    n_copies = [
        remote(ncomb.at[lax.rem(z + d, nz)], ndst.at[d - 1], nzs.at[d - 1], nzr.at[d - 1], z_peer(d))
        for d in range(1, nz)
    ]
    for c in n_copies[:-1]:
        c.start()

    for c in f_copies:
        c.wait_recv()

    chunk = f // 2
    plane_rows = pbuf.shape[2]
    piece = zbuf.shape[2]
    sent = [[] for _ in range(relations)]
    batches = [[None] * relations for _ in range(5)]

    def launch(stage, r, copies):
        for c in copies:
            c.start()
        batches[stage][r] = copies
        sent[r].extend(copies)

    def arrived(stage, r):
        for c in batches[stage][r]:
            c.wait_recv()

    def terms(r):
        for h in range(2):
            y = jnp.dot(
                a[r * tn : (r + 1) * tn, :],
                xall[:, h * chunk : (h + 1) * chunk],
                preferred_element_type=F32,
            )
            dw[r, h] = jnp.dot(y.astype(BF16).T, g[...], preferred_element_type=F32)
        launch(0, r, [remote(dw.at[r, other], dwrecv.at[r], ds.at[r, 0], dr.at[r, 0], sibling)])

    def plane_scatter(r):
        arrived(0, r)
        for k in range(nr):
            rows = slice(k * plane_rows, (k + 1) * plane_rows)
            pbuf[r, k] = (dw[r, core, rows, :] + dwrecv[r, rows, :]).astype(BF16)
        launch(1, r, [
            remote(
                pbuf.at[r, lax.rem(me_r + d, nr)], precv.at[r, d - 1],
                ps.at[r, d - 1], pr.at[r, d - 1], row_peer(d),
            )
            for d in range(1, nr)
        ])

    def z_scatter(r):
        arrived(1, r)
        for k in range(nz):
            rows = slice(k * piece, (k + 1) * piece)
            part = pbuf[r, me_r, rows, :].astype(F32)
            for d in range(1, nr):
                part = part + precv[r, d - 1, rows, :].astype(F32)
            zbuf[r, k] = part.astype(BF16)
        launch(2, r, [
            remote(
                zbuf.at[r, lax.rem(z + d, nz)], zrecv.at[r, d - 1],
                zs.at[r, d - 1], zr.at[r, d - 1], z_peer(d),
            )
            for d in range(1, nz)
        ])

    def z_gather(r):
        arrived(2, r)
        final = zbuf[r, z].astype(F32)
        for d in range(1, nz):
            final = final + zrecv[r, d - 1].astype(F32)
        ag_ref[r, core, me_r, z] = final.astype(BF16)
        mine = ag_ref.at[r, core, me_r, z]
        launch(3, r, [remote(mine, mine, azs.at[r, d - 1], azr.at[r, d - 1], z_peer(d)) for d in range(1, nz)])

    last = [[] for _ in range(relations)]

    def plane_gather(r):
        arrived(3, r)
        mine = ag_ref.at[r, core, me_r]
        launch(4, r, [remote(mine, mine, aps.at[r, d - 1], apr.at[r, d - 1], row_peer(d)) for d in range(1, nr)])
        c = remote(mine, mine, acs.at[r, 0], acr.at[r, 0], sibling)
        c.start()
        last[r].append(c)

    def core_gather(r):
        for d in range(1, nr):
            batches[4][r][d - 1].wait_recv()
            slot = ag_ref.at[r, core, lax.rem(me_r + nr - d, nr)]
            c = remote(slot, slot, acs.at[r, d], acr.at[r, d], sibling)
            c.start()
            last[r].append(c)

    terms(0)
    for r in range(1, relations):
        terms(r)
        plane_scatter(r - 1)
    plane_scatter(relations - 1)
    stages = (z_scatter, z_gather, plane_gather, core_gather)
    for t in range(relations + len(stages) - 1):
        for stage in reversed(range(len(stages))):
            if 0 <= t - stage < relations:
                stages[stage](t - stage)
        if t == relations:
            n_copies[-1].start()

    for c in n_copies:
        c.wait_recv()
    own = nsend[core, z] + nrecv[z]
    for d in range(1, nz):
        own = own + ndst[d - 1].astype(F32)
    dn_ref[...] = own.T.astype(BF16)

    for r in range(relations):
        for c in last[r]:
            c.wait_recv()
        for c in sent[r] + last[r]:
            c.wait_send()
    for c in g_copies + x_copies + f_copies + [n_core] + n_copies:
        c.wait_send()


def widen_kernel(dn_ref, dw_ref, dn_out, dw_out, nodes, narrow, wide, in_sem, out_sem):
    parts, rows = narrow.shape[0], narrow.shape[1]

    def part(ref, k):
        return ref.at[k * rows : (k + 1) * rows, :]

    loads = [pltpu.make_async_copy(part(dw_ref, k), narrow.at[k], in_sem.at[k]) for k in range(parts)]
    stores = [pltpu.make_async_copy(wide.at[k], part(dw_out, k), out_sem.at[k]) for k in range(parts)]
    loads.append(pltpu.make_async_copy(dn_ref, nodes, in_sem.at[parts]))
    stores.append(pltpu.make_async_copy(nodes, dn_out, out_sem.at[parts]))
    for c in loads:
        c.start()
    for k in range(parts):
        loads[k].wait()
        wide[k] = narrow[k].astype(F32)
        stores[k].start()
    loads[parts].wait()
    stores[parts].start()
    for c in stores:
        c.wait()


def widen(d_nodes, gathered):
    total, f = gathered.shape
    parts = 6 if total % 96 == 0 else 1
    rows = total // parts
    hbm = pl.BlockSpec(memory_space=pltpu.HBM)
    return pl.pallas_call(
        widen_kernel,
        in_specs=[hbm, hbm],
        out_specs=(hbm, hbm),
        out_shape=(
            jax.ShapeDtypeStruct(d_nodes.shape, BF16),
            jax.ShapeDtypeStruct(gathered.shape, F32),
        ),
        scratch_shapes=[
            pltpu.VMEM(d_nodes.shape, BF16),
            pltpu.VMEM((parts, rows, f), BF16),
            pltpu.VMEM((parts, rows, f), F32),
            pltpu.SemaphoreType.DMA((parts + 1,)),
            pltpu.SemaphoreType.DMA((parts + 1,)),
        ],
    )(d_nodes, gathered)


def body(nr, nc, out_grad, node_in, weights, tile_vals, tile_rows, tile_cols, tile_count):
    relations, f = weights.shape[0], weights.shape[1]
    tn, width = out_grad.shape
    nd = node_in.shape[0]
    sn = nd * nc
    nz = nc // 2
    half = f // 2
    plane_rows = half // nr
    piece = plane_rows // nz
    dense = assemble(tile_vals, tile_rows, tile_cols, tile_count, tn, sn)
    dma = lambda *n: pltpu.SemaphoreType.DMA(n)
    vmem = pl.BlockSpec(memory_space=pltpu.VMEM)
    hbm = pl.BlockSpec(memory_space=pltpu.HBM)
    d_nodes, gathered = pl.pallas_call(
        functools.partial(main_kernel, nr, nc, relations),
        out_shape=(
            jax.ShapeDtypeStruct((nd, f), BF16),
            jax.ShapeDtypeStruct((relations, 2, nr, nz, piece, f), BF16),
        ),
        in_specs=[vmem, vmem, hbm, hbm],
        out_specs=(vmem, vmem),
        scratch_shapes=[
            pltpu.VMEM((nr, tn, width), BF16),
            pltpu.VMEM((tn, f), BF16),
            pltpu.VMEM(weights.shape, BF16),
            pltpu.VMEM((relations * tn, sn), BF16),
            pltpu.VMEM((sn, f), BF16),
            pltpu.VMEM((f, relations * tn), BF16),
            pltpu.VMEM((2, nz, f, nd), F32),
            pltpu.VMEM((nz, f, nd), F32),
            pltpu.VMEM((nz, f, nd), BF16),
            pltpu.VMEM((nz - 1, f, nd), BF16),
            pltpu.VMEM((relations, 2, half, f), F32),
            pltpu.VMEM((relations, half, f), F32),
            pltpu.VMEM((relations, nr, plane_rows, f), BF16),
            pltpu.VMEM((relations, nr - 1, plane_rows, f), BF16),
            pltpu.VMEM((relations, nz, piece, f), BF16),
            pltpu.VMEM((relations, nz - 1, piece, f), BF16),
            dma(2),
            dma(nr - 1), dma(nr - 1),
            dma(nz - 1), dma(nz - 1),
            dma(nz), dma(nz),
            dma(1), dma(1),
            dma(nz - 1), dma(nz - 1),
            dma(relations, 1), dma(relations, 1),
            dma(relations, nr - 1), dma(relations, nr - 1),
            dma(relations, nz - 1), dma(relations, nz - 1),
            dma(relations, nz - 1), dma(relations, nz - 1),
            dma(relations, nr - 1), dma(relations, nr - 1),
            dma(relations, nr), dma(relations, nr),
        ],
        compiler_params=pltpu.CompilerParams(
            collective_id=0, has_side_effects=True, vmem_limit_bytes=67043328
        ),
    )(out_grad, node_in, weights, dense)
    d_nodes, d_weights = widen(d_nodes, gathered.reshape(relations * f, f))
    return d_nodes, d_weights.reshape(relations, f, f)


def solution(mesh):
    return jax.shard_map(
        functools.partial(body, mesh.shape["row"], mesh.shape["col"]),
        mesh=mesh,
        in_specs=(
            P("col", "row"),
            P(("row", "col"), None),
            P(),
            P(None, "col", "row", None, None, None),
            P(None, "col", "row", None),
            P(None, "col", "row", None),
            P(None, "col", "row"),
        ),
        out_specs=(P(("row", "col"), None), P()),
        check_vma=False,
    )
```

```python
import functools

import jax
import jax.numpy as jnp
from jax import lax
from jax.experimental import pallas as pl
from jax.experimental.pallas import tpu as pltpu
from jax.sharding import PartitionSpec as P

MESH = pl.DeviceIdType.MESH
F32 = jnp.float32
BF16 = jnp.bfloat16


def assemble_kernel(rows_ref, cols_ref, count_ref, tiles_ref, out_ref, total):
    relation = pl.program_id(0)
    tile_rows, tile_cols, tile = total.shape[0], total.shape[1], total.shape[2]
    for i in range(tile_rows):
        for j in range(tile_cols):
            total[i, j] = jnp.zeros((tile, tile), F32)

    def add_tile(slot, carry):
        i = rows_ref[relation, 0, 0, slot]
        j = cols_ref[relation, 0, 0, slot]
        total[i, j] = total[i, j] + tiles_ref[0, slot].astype(F32)
        return carry

    lax.fori_loop(0, count_ref[relation], add_tile, 0)
    for i in range(tile_rows):
        for j in range(tile_cols):
            out_ref[i * tile : (i + 1) * tile, j * tile : (j + 1) * tile] = total[i, j].astype(BF16)


def assemble(tile_vals, tile_rows, tile_cols, tile_count, targets, sources):
    relations, cap, tile = tile_vals.shape[0], tile_vals.shape[3], tile_vals.shape[4]
    vals = tile_vals.reshape(relations, cap, tile, tile)
    return pl.pallas_call(
        assemble_kernel,
        grid_spec=pltpu.PrefetchScalarGridSpec(
            num_scalar_prefetch=3,
            grid=(relations,),
            in_specs=[pl.BlockSpec((1, cap, tile, tile), lambda r, *_: (r, 0, 0, 0))],
            out_specs=pl.BlockSpec((targets, sources), lambda r, *_: (r, 0)),
            scratch_shapes=[pltpu.VMEM((targets // tile, sources // tile, tile, tile), F32)],
        ),
        out_shape=jax.ShapeDtypeStruct((relations * targets, sources), BF16),
        compiler_params=pltpu.CompilerParams(vmem_limit_bytes=60 * 2**20),
    )(
        tile_rows,
        tile_cols,
        tile_count.reshape(relations),
        vals,
    )


def main_kernel(
    nr, nc, relations,
    grad_ref, nodes_ref, w_hbm, a_hbm,
    dn_ref, ag_ref,
    gslot, g, w, a, xall, pt, nsend, nrecv, ncomb, ndst,
    dw, dwrecv, pbuf, precv, zbuf, zrecv,
    load_sem, gs, gr, xs, xr, fs, fr, ns, nrs, nzs, nzr, ds, dr, ps, pr, zs, zr,
    azs, azr, aps, apr, acs, acr,
):
    nz = nc // 2
    tn = grad_ref.shape[0]
    width = grad_ref.shape[1]
    nd = nodes_ref.shape[0]
    f = w_hbm.shape[1]
    me_r = lax.axis_index("row")
    me_c = lax.axis_index("col")
    z = me_c // 2
    core = me_c % 2
    other = 1 - core
    sibling = {"col": z * 2 + other}

    def row_peer(d):
        return {"row": lax.rem(me_r + d, nr)}

    def z_peer(d):
        return {"col": lax.rem(z + d, nz) * 2 + core}

    def remote(src, dst, send, recv, dev):
        return pltpu.make_async_remote_copy(
            src_ref=src, dst_ref=dst, send_sem=send, recv_sem=recv, device_id=dev, device_id_type=MESH
        )

    def x_slot(k):
        return xall.at[pl.ds(pl.multiple_of(k * nd, nd), nd), :]

    load_a = pltpu.make_async_copy(a_hbm, a, load_sem.at[0])
    load_w = pltpu.make_async_copy(w_hbm, w, load_sem.at[1])
    load_w.start()
    load_a.start()

    barrier = pltpu.get_barrier_semaphore()
    for d in range(1, nr):
        pl.semaphore_signal(barrier, inc=1, device_id=row_peer(d), device_id_type=MESH)
    for d in range(1, nz):
        pl.semaphore_signal(barrier, inc=1, device_id=z_peer(d), device_id_type=MESH)
    pl.semaphore_signal(barrier, inc=1, device_id=sibling, device_id_type=MESH)
    pl.semaphore_wait(barrier, nr - 1 + nz - 1 + 1)

    g_copies = [
        remote(grad_ref, gslot.at[me_r], gs.at[d - 1], gr.at[d - 1], row_peer(d)) for d in range(1, nr)
    ]
    for c in g_copies:
        c.start()
    x_copies = [
        remote(nodes_ref, x_slot(me_c), xs.at[d - 1], xr.at[d - 1], z_peer(d)) for d in range(1, nz)
    ]
    for c in x_copies:
        c.start()
    f_copies = [remote(nodes_ref, x_slot(me_c), fs.at[0], fr.at[0], sibling)]
    f_copies[0].start()
    xall[pl.ds(pl.multiple_of(me_c * nd, nd), nd), :] = nodes_ref[...]
    gslot[me_r] = grad_ref[...]

    load_w.wait()
    for c in g_copies:
        c.wait_recv()
    for k in range(nr):
        g[:, k * width : (k + 1) * width] = gslot[k]
    for r in range(relations):
        pt[:, r * tn : (r + 1) * tn] = lax.dot_general(
            w[r], g[...], (((1,), (1,)), ((), ())), preferred_element_type=F32
        ).astype(BF16)
    load_a.wait()

    def mix(k, carry):
        cols = pl.ds(pl.multiple_of(k * 2 * nd, 2 * nd), 2 * nd)
        both = jnp.dot(pt[...], a[:, cols], preferred_element_type=F32)
        nsend[0, k] = both[:, :nd]
        nsend[1, k] = both[:, nd:]
        return carry

    lax.fori_loop(0, nz, mix, 0)
    n_core = remote(nsend.at[other], nrecv, ns.at[0], nrs.at[0], sibling)
    n_core.start()

    for d in range(1, nz):
        x_copies[d - 1].wait_recv()
        slot = lax.rem(z + nz - d, nz) * 2 + core
        c = remote(x_slot(slot), x_slot(slot), fs.at[d], fr.at[d], sibling)
        c.start()
        f_copies.append(c)

    n_core.wait_recv()

    def combine(k, carry):
        ncomb[k] = (nsend[core, k] + nrecv[k]).astype(BF16)
        return carry

    lax.fori_loop(0, nz, combine, 0)
    n_copies = [
        remote(ncomb.at[lax.rem(z + d, nz)], ndst.at[d - 1], nzs.at[d - 1], nzr.at[d - 1], z_peer(d))
        for d in range(1, nz)
    ]
    for c in n_copies[:-1]:
        c.start()

    for c in f_copies:
        c.wait_recv()

    chunk = f // 2
    plane_rows = pbuf.shape[2]
    piece = zbuf.shape[2]
    sent = [[] for _ in range(relations)]
    batches = [[None] * relations for _ in range(5)]

    def launch(stage, r, copies):
        for c in copies:
            c.start()
        batches[stage][r] = copies
        sent[r].extend(copies)

    def arrived(stage, r):
        for c in batches[stage][r]:
            c.wait_recv()

    def terms(r):
        for h in range(2):
            y = jnp.dot(
                a[r * tn : (r + 1) * tn, :],
                xall[:, h * chunk : (h + 1) * chunk],
                preferred_element_type=F32,
            )
            dw[r, h] = jnp.dot(y.astype(BF16).T, g[...], preferred_element_type=F32)
        launch(0, r, [remote(dw.at[r, other], dwrecv.at[r], ds.at[r, 0], dr.at[r, 0], sibling)])

    def plane_scatter(r):
        arrived(0, r)
        for k in range(nr):
            rows = slice(k * plane_rows, (k + 1) * plane_rows)
            pbuf[r, k] = (dw[r, core, rows, :] + dwrecv[r, rows, :]).astype(BF16)
        launch(1, r, [
            remote(
                pbuf.at[r, lax.rem(me_r + d, nr)], precv.at[r, d - 1],
                ps.at[r, d - 1], pr.at[r, d - 1], row_peer(d),
            )
            for d in range(1, nr)
        ])

    def z_scatter(r):
        arrived(1, r)
        for k in range(nz):
            rows = slice(k * piece, (k + 1) * piece)
            part = pbuf[r, me_r, rows, :].astype(F32)
            for d in range(1, nr):
                part = part + precv[r, d - 1, rows, :].astype(F32)
            zbuf[r, k] = part.astype(BF16)
        launch(2, r, [
            remote(
                zbuf.at[r, lax.rem(z + d, nz)], zrecv.at[r, d - 1],
                zs.at[r, d - 1], zr.at[r, d - 1], z_peer(d),
            )
            for d in range(1, nz)
        ])

    def z_gather(r):
        arrived(2, r)
        final = zbuf[r, z].astype(F32)
        for d in range(1, nz):
            final = final + zrecv[r, d - 1].astype(F32)
        ag_ref[r, core, me_r, z] = final.astype(BF16)
        mine = ag_ref.at[r, core, me_r, z]
        launch(3, r, [remote(mine, mine, azs.at[r, d - 1], azr.at[r, d - 1], z_peer(d)) for d in range(1, nz)])

    last = [[] for _ in range(relations)]

    def plane_gather(r):
        arrived(3, r)
        mine = ag_ref.at[r, core, me_r]
        launch(4, r, [remote(mine, mine, aps.at[r, d - 1], apr.at[r, d - 1], row_peer(d)) for d in range(1, nr)])
        c = remote(mine, mine, acs.at[r, 0], acr.at[r, 0], sibling)
        c.start()
        last[r].append(c)

    def core_gather(r):
        for d in range(1, nr):
            batches[4][r][d - 1].wait_recv()
            slot = ag_ref.at[r, core, lax.rem(me_r + nr - d, nr)]
            c = remote(slot, slot, acs.at[r, d], acr.at[r, d], sibling)
            c.start()
            last[r].append(c)

    terms(0)
    for r in range(1, relations):
        terms(r)
        plane_scatter(r - 1)
    plane_scatter(relations - 1)
    stages = (z_scatter, z_gather, plane_gather, core_gather)
    for t in range(relations + len(stages) - 1):
        for stage in range(len(stages)):
            if 0 <= t - stage < relations:
                stages[stage](t - stage)
        if t == relations:
            n_copies[-1].start()

    for c in n_copies:
        c.wait_recv()
    own = nsend[core, z] + nrecv[z]
    for d in range(1, nz):
        own = own + ndst[d - 1].astype(F32)
    dn_ref[...] = own.T.astype(BF16)

    for r in range(relations):
        for c in last[r]:
            c.wait_recv()
        for c in sent[r] + last[r]:
            c.wait_send()
    for c in g_copies + x_copies + f_copies + [n_core] + n_copies:
        c.wait_send()


def widen_kernel(dn_ref, dw_ref, dn_out, dw_out, nodes, narrow, wide, in_sem, out_sem):
    parts, rows = narrow.shape[0], narrow.shape[1]

    def part(ref, k):
        return ref.at[k * rows : (k + 1) * rows, :]

    loads = [pltpu.make_async_copy(part(dw_ref, k), narrow.at[k], in_sem.at[k]) for k in range(parts)]
    stores = [pltpu.make_async_copy(wide.at[k], part(dw_out, k), out_sem.at[k]) for k in range(parts)]
    loads.append(pltpu.make_async_copy(dn_ref, nodes, in_sem.at[parts]))
    stores.append(pltpu.make_async_copy(nodes, dn_out, out_sem.at[parts]))
    for c in loads:
        c.start()
    for k in range(parts):
        loads[k].wait()
        wide[k] = narrow[k].astype(F32)
        stores[k].start()
    loads[parts].wait()
    stores[parts].start()
    for c in stores:
        c.wait()


def widen(d_nodes, gathered):
    total, f = gathered.shape
    parts = 6 if total % 96 == 0 else 1
    rows = total // parts
    hbm = pl.BlockSpec(memory_space=pltpu.HBM)
    return pl.pallas_call(
        widen_kernel,
        in_specs=[hbm, hbm],
        out_specs=(hbm, hbm),
        out_shape=(
            jax.ShapeDtypeStruct(d_nodes.shape, BF16),
            jax.ShapeDtypeStruct(gathered.shape, F32),
        ),
        scratch_shapes=[
            pltpu.VMEM(d_nodes.shape, BF16),
            pltpu.VMEM((parts, rows, f), BF16),
            pltpu.VMEM((parts, rows, f), F32),
            pltpu.SemaphoreType.DMA((parts + 1,)),
            pltpu.SemaphoreType.DMA((parts + 1,)),
        ],
    )(d_nodes, gathered)


def body(nr, nc, out_grad, node_in, weights, tile_vals, tile_rows, tile_cols, tile_count):
    relations, f = weights.shape[0], weights.shape[1]
    tn, width = out_grad.shape
    nd = node_in.shape[0]
    sn = nd * nc
    nz = nc // 2
    half = f // 2
    plane_rows = half // nr
    piece = plane_rows // nz
    dense = assemble(tile_vals, tile_rows, tile_cols, tile_count, tn, sn)
    dma = lambda *n: pltpu.SemaphoreType.DMA(n)
    vmem = pl.BlockSpec(memory_space=pltpu.VMEM)
    hbm = pl.BlockSpec(memory_space=pltpu.HBM)
    d_nodes, gathered = pl.pallas_call(
        functools.partial(main_kernel, nr, nc, relations),
        out_shape=(
            jax.ShapeDtypeStruct((nd, f), BF16),
            jax.ShapeDtypeStruct((relations, 2, nr, nz, piece, f), BF16),
        ),
        in_specs=[vmem, vmem, hbm, hbm],
        out_specs=(vmem, vmem),
        scratch_shapes=[
            pltpu.VMEM((nr, tn, width), BF16),
            pltpu.VMEM((tn, f), BF16),
            pltpu.VMEM(weights.shape, BF16),
            pltpu.VMEM((relations * tn, sn), BF16),
            pltpu.VMEM((sn, f), BF16),
            pltpu.VMEM((f, relations * tn), BF16),
            pltpu.VMEM((2, nz, f, nd), F32),
            pltpu.VMEM((nz, f, nd), F32),
            pltpu.VMEM((nz, f, nd), BF16),
            pltpu.VMEM((nz - 1, f, nd), BF16),
            pltpu.VMEM((relations, 2, half, f), F32),
            pltpu.VMEM((relations, half, f), F32),
            pltpu.VMEM((relations, nr, plane_rows, f), BF16),
            pltpu.VMEM((relations, nr - 1, plane_rows, f), BF16),
            pltpu.VMEM((relations, nz, piece, f), BF16),
            pltpu.VMEM((relations, nz - 1, piece, f), BF16),
            dma(2),
            dma(nr - 1), dma(nr - 1),
            dma(nz - 1), dma(nz - 1),
            dma(nz), dma(nz),
            dma(1), dma(1),
            dma(nz - 1), dma(nz - 1),
            dma(relations, 1), dma(relations, 1),
            dma(relations, nr - 1), dma(relations, nr - 1),
            dma(relations, nz - 1), dma(relations, nz - 1),
            dma(relations, nz - 1), dma(relations, nz - 1),
            dma(relations, nr - 1), dma(relations, nr - 1),
            dma(relations, nr), dma(relations, nr),
        ],
        compiler_params=pltpu.CompilerParams(
            collective_id=0, has_side_effects=True, vmem_limit_bytes=67043328
        ),
    )(out_grad, node_in, weights, dense)
    d_nodes, d_weights = widen(d_nodes, gathered.reshape(relations * f, f))
    return d_nodes, d_weights.reshape(relations, f, f)


def solution(mesh):
    return jax.shard_map(
        functools.partial(body, mesh.shape["row"], mesh.shape["col"]),
        mesh=mesh,
        in_specs=(
            P("col", "row"),
            P(("row", "col"), None),
            P(),
            P(None, "col", "row", None, None, None),
            P(None, "col", "row", None),
            P(None, "col", "row", None),
            P(None, "col", "row"),
        ),
        out_specs=(P(("row", "col"), None), P()),
        check_vma=False,
    )
```
